32 devices in a mesh: gx: 8 (over z, y), gy: 2 (over x), ha: 2 (over core).
Axes of the slice: x: 2, y: 2, z: 4, core: 2. Of those that a mesh axis runs over, the one named last changes fastest.
Arguments:
- coupling: bfloat16 [8, 4, 4, 768, 768], P('gx', ('gy', 'ha')), may hold values from -0.125 to 0.125
- interior_inverse: bfloat16 [8, 4, 4, 768, 768], P('gx', ('gy', 'ha')), as said below
- boundary_stiffness: bfloat16 [8, 4, 768, 768], P('gx', ('gy', 'ha')), as said below
- block_counts: int32 [8, 4], P('gx', ('gy', 'ha')), may hold values from 1 to 4, as said below
- initial_traces: float32 [8, 4, 768, 128], P('gx', ('gy', 'ha')), may hold values from -2 to 2
- trace_loads: float32 [8, 4, 768, 128], P('gx', ('gy', 'ha')), may hold values from -18 to 18
Outputs:
- traces: float32 [8, 4, 768, 128], P('gx', ('gy', 'ha'))
- residual: float32 [8, 4, 768, 128], P('gx', ('gy', 'ha'))
The draws below stay inside these ranges and needn't reach their ends.
Inputs may be any that keep to these rules, and one draw needn't show every extreme that they name: `block_counts`: the two cells in columns 2m and 2m+1 of one grid row hold at most 5 blocks together; some cell holds 4. `interior_inverse`: symmetric in its last two dimensions. `boundary_stiffness`: symmetric in its last two dimensions.
All inputs are finite; a program needn't handle non-finite values.
Results may differ from the reference program's by a relative error of at most 0.00095.
Values may be sent and summed in bfloat16 or wider, within the bound.
A program may use at most 128 MiB of HBM per device.

```python
import jax
import jax.numpy as jnp
from jax import lax

MODES = 128
FACES = 6
TR = 768
INTR = 768
SLOTS = 4
LOADS = 128
SWEEPS = 3
NX = 8
NYC = 4


def symmetric_noise(key, shape, spread):
    noise = jnp.clip(jax.random.normal(key, shape, jnp.float32), -4.0, 4.0) * spread
    return (noise + jnp.swapaxes(noise, -1, -2)) / jnp.sqrt(2.0)


def draw_interior_inverse(key, part):
    key_noise = jax.random.fold_in(jax.random.fold_in(key, 11), 0)
    shape = (NX, NYC, SLOTS, INTR, INTR)
    symmetric = symmetric_noise(key_noise, shape, 0.25 / INTR ** 0.5)
    diagonal = jnp.ones(shape[:-1], jnp.float32)
    identity = jnp.eye(INTR, dtype=jnp.float32)
    return (symmetric + diagonal[..., None] * identity).astype(jnp.bfloat16)


def draw_boundary_stiffness(key, part):
    key_noise = jax.random.fold_in(jax.random.fold_in(key, 23), 0)
    shape = (NX, NYC, TR, TR)
    symmetric = symmetric_noise(key_noise, shape, 1.5 / TR ** 0.5)
    diagonal = jnp.full(shape[:-1], 7.0, jnp.float32)
    identity = jnp.eye(TR, dtype=jnp.float32)
    return (symmetric + diagonal[..., None] * identity).astype(jnp.bfloat16)


def draw_block_counts(key, part):
    key_first, key_second, key_flip = jax.random.split(jax.random.fold_in(key, 37), 3)
    pair_shape = (NX, NYC // 2)
    first_count = jax.random.randint(key_first, pair_shape, 1, 5)
    second_count = jax.random.randint(key_second, pair_shape, 1, 6 - first_count)
    flipped = jax.random.randint(key_flip, pair_shape, 0, 2)
    lower_cell = jnp.where(flipped == 1, second_count, first_count)
    upper_cell = jnp.where(flipped == 1, first_count, second_count)
    lower_cell = lower_cell.at[0, 0].set(4)
    upper_cell = upper_cell.at[0, 0].set(1)
    return jnp.stack([lower_cell, upper_cell], -1).reshape(NX, NYC).astype(jnp.int32)


def block_levels(rng, extent, shards, least, high):
    def one(position, blocks):
        heights = jax.random.uniform(jax.random.fold_in(jax.random.fold_in(rng, 6), position), (blocks,), jnp.float32, least / len(shards), high / len(shards))
        return jnp.repeat(jnp.exp(heights), extent[position] // blocks).reshape((-1,) + (1,) * (len(extent) - position - 1))

    level = one(*shards[0])
    for cut in shards[1:]:
        level = level * one(*cut)
    return level


def normal_values(own_key, extent, width, most, shards=(), kind=jnp.bfloat16):
    gain = block_levels(own_key, extent, shards, -0.22, 0.18) if shards else 1.0
    result = jax.random.normal(own_key, extent, jnp.float32) * width * gain
    return jnp.minimum(jnp.maximum(result, -most), most).astype(kind)


def setup_inputs(seed: int = 0) -> dict:
    seeds = jax.random.split(jax.random.key(seed), 7)
    coupling = normal_values(seeds[0], (NX, NYC, SLOTS, TR, INTR), (3 * INTR) ** -0.5, 0.125, ((0, 8), (1, 4)))
    interior_inverse = draw_interior_inverse(jax.random.fold_in(seeds[6], 71), 0)
    boundary_stiffness = draw_boundary_stiffness(jax.random.fold_in(seeds[6], 71), 0)
    block_counts = draw_block_counts(jax.random.fold_in(seeds[6], 71), 0)
    initial_traces = normal_values(seeds[4], (NX, NYC, TR, LOADS), 0.3, 2.0, ((0, 8), (1, 4)), jnp.float32)
    trace_loads = normal_values(seeds[5], (NX, NYC, TR, LOADS), 3.0, 18.0, ((0, 8), (1, 4)), jnp.float32)
    return {"coupling": coupling, "interior_inverse": interior_inverse, "boundary_stiffness": boundary_stiffness, "block_counts": block_counts, "initial_traces": initial_traces, "trace_loads": trace_loads}


penalty_weight = 2.0
lower_bound = 1.0
upper_bound = 14.0
spectrum_centre = (upper_bound + lower_bound) / 2.0
spectrum_half = (upper_bound - lower_bound) / 2.0
sigma_ratio = spectrum_centre / spectrum_half


def schur_block(coupling_block, inverse_block):
    product = jnp.dot(coupling_block, inverse_block, preferred_element_type=jnp.float32).astype(jnp.bfloat16)
    return jnp.dot(product, coupling_block.T, preferred_element_type=jnp.float32)


def condense_cell(packed):
    coupling, inverse, stiffness, blocks = packed
    condensed = stiffness.astype(jnp.float32)
    for slot_index in range(SLOTS):
        term = lax.cond(blocks > slot_index,
                        lambda: schur_block(coupling[slot_index], inverse[slot_index]),
                        lambda: jnp.zeros((TR, TR), jnp.float32))
        condensed = condensed - term
    return condensed


def apply_operator(condensed, traces):
    coupled = jnp.einsum("abij,abjl->abil", condensed, traces, precision=lax.Precision.HIGHEST)
    face_traces = traces.reshape(NX, NYC, FACES, MODES, LOADS)
    nothing_row = jnp.zeros((1, NYC, MODES, LOADS), jnp.float32)
    nothing_col = jnp.zeros((NX, 1, MODES, LOADS), jnp.float32)
    from_below_x = jnp.concatenate([nothing_row, face_traces[:-1, :, 1]], 0)
    from_above_x = jnp.concatenate([face_traces[1:, :, 0], nothing_row], 0)
    from_below_y = jnp.concatenate([nothing_col, face_traces[:, :-1, 3]], 1)
    from_above_y = jnp.concatenate([face_traces[:, 1:, 2], nothing_col], 1)
    absent = jnp.zeros_like(from_below_x)
    neighbours = jnp.stack([from_below_x, from_above_x, from_below_y, from_above_y, absent, absent], 2)
    neighbours = neighbours.reshape(NX, NYC, TR, LOADS)
    return coupled + penalty_weight * (traces - neighbours)


def reference(coupling, interior_inverse, boundary_stiffness, block_counts, initial_traces, trace_loads):
    cell_total = NX * NYC
    condensed = lax.map(condense_cell, (coupling.reshape(cell_total, SLOTS, TR, INTR),
                                        interior_inverse.reshape(cell_total, SLOTS, INTR, INTR),
                                        boundary_stiffness.reshape(cell_total, TR, TR),
                                        block_counts.reshape(cell_total)))
    condensed = condensed.reshape(NX, NYC, TR, TR)
    traces = initial_traces
    residual = trace_loads - apply_operator(condensed, traces)
    direction = residual / spectrum_centre
    weight_old = 1.0 / sigma_ratio
    for sweep_index in range(SWEEPS):
        traces = traces + direction
        residual = trace_loads - apply_operator(condensed, traces)
        if sweep_index + 1 < SWEEPS:
            weight_new = 1.0 / (2.0 * sigma_ratio - weight_old)
            direction = weight_new * weight_old * direction + (2.0 * weight_new / spectrum_half) * residual
            weight_old = weight_new
    return traces, residual
```

```python
import functools

import jax
import jax.numpy as jnp
from jax import lax
from jax.experimental import pallas as pl
from jax.experimental.pallas import tpu as pltpu
from jax.sharding import PartitionSpec as P

SWEEPS = 3
FACES = 6

penalty_weight = 2.0
lower_bound = 1.0
upper_bound = 14.0
spectrum_centre = (upper_bound + lower_bound) / 2.0
spectrum_half = (upper_bound - lower_bound) / 2.0
sigma_ratio = spectrum_centre / spectrum_half


def sweep_weights():
    weights = [(0.0, 1.0 / spectrum_centre)]
    weight_old = 1.0 / sigma_ratio
    for _ in range(SWEEPS - 1):
        weight_new = 1.0 / (2.0 * sigma_ratio - weight_old)
        weights.append((weight_new * weight_old, 2.0 * weight_new / spectrum_half))
        weight_old = weight_new
    return weights


def two_parts(value):
    high = value.astype(jnp.bfloat16)
    low = (value - high.astype(jnp.float32)).astype(jnp.bfloat16)
    return high, low


def product(left, right, dims):
    return lax.dot_general(left, right, (dims, ((), ())), preferred_element_type=jnp.float32)


def kernel(
    axis_sizes,
    coupling,
    inverse,
    stiffness,
    live,
    initial,
    loads,
    traces_out,
    residual_out,
    wide,
    inv,
    factors,
    turned,
    inner,
    held,
    bound,
    direction,
    landed,
    in_sems,
    send_sems,
    recv_sems,
):
    slots, trace_width, inner_width = coupling.shape
    load_width = initial.shape[1]
    mode_width = trace_width // FACES
    rows, groups, halves = axis_sizes
    columns = groups * halves
    row = lax.axis_index("gx")
    column = lax.axis_index("gy") * halves + lax.axis_index("ha")

    def column_id(index):
        return {"gy": lax.div(index, halves), "ha": lax.rem(index, halves)}

    routes = (
        (1, 0, row + 1 < rows, {"gx": row + 1}),
        (0, 1, row > 0, {"gx": row - 1}),
        (3, 2, column + 1 < columns, column_id(column + 1)),
        (2, 3, column > 0, column_id(column - 1)),
    )
    arrivals = ((0, row > 0), (1, row + 1 < rows), (2, column > 0), (3, column + 1 < columns))

    copies = [
        pltpu.make_async_copy(initial, held, in_sems.at[0]),
        pltpu.make_async_copy(loads, bound, in_sems.at[1]),
        pltpu.make_async_copy(stiffness, wide.at[:, pl.ds(0, trace_width)], in_sems.at[2]),
    ]
    coupling_copies, inverse_copies = [], []
    for slot in range(slots):
        spot = pl.ds(trace_width + slot * inner_width, inner_width)
        coupling_copies.append(
            pltpu.make_async_copy(coupling.at[slot], wide.at[:, spot], in_sems.at[3 + slot])
        )
        inverse_copies.append(
            pltpu.make_async_copy(inverse.at[slot], inv.at[slot], in_sems.at[3 + slots + slot])
        )
    copies[0].start()
    for slot in range(slots):
        coupling_copies[slot].start()
        inverse_copies[slot].start()
    copies[2].start()
    copies[1].start()

    barrier = pltpu.get_barrier_semaphore()
    partners = 0
    for _, _, exists, target in routes:
        partners = partners + exists.astype(jnp.int32)

        @pl.when(exists)
        def _():
            pl.semaphore_signal(barrier, inc=1, device_id=target, device_id_type=pl.DeviceIdType.MESH)

    for face, exists in arrivals:

        @pl.when(jnp.logical_not(exists))
        def _():
            landed[:, face] = jnp.zeros((SWEEPS + 1, mode_width, load_width), jnp.float32)

    pl.semaphore_wait(barrier, partners)

    def outgoing(step, route):
        face, spot, _, target = route
        return pltpu.make_async_remote_copy(
            src_ref=held.at[pl.ds(face * mode_width, mode_width)],
            dst_ref=landed.at[step, spot],
            send_sem=send_sems.at[face],
            recv_sem=recv_sems.at[step, spot],
            device_id=target,
            device_id_type=pl.DeviceIdType.MESH,
        )

    def send(step, route):
        @pl.when(route[2])
        def _():
            outgoing(step, route).start()

    def wait_sent(step):
        for route in routes:

            @pl.when(route[2])
            def _():
                outgoing(step, route).wait_send()

    def wait_arrived(step):
        for (face, exists), route in zip(arrivals, routes):

            @pl.when(exists)
            def _():
                outgoing(step, route).wait_recv()

    def keep_parts(traces):
        high, low = two_parts(traces)
        factors[pl.ds(0, trace_width), pl.ds(0, load_width)] = high
        factors[pl.ds(0, trace_width), pl.ds(load_width, load_width)] = low
        high, low = two_parts(traces.T)
        turned[pl.ds(0, load_width)] = high
        turned[pl.ds(load_width, load_width)] = low

    def apply(first):
        for slot in range(slots):
            spot = pl.ds(trace_width + slot * inner_width, inner_width)
            if first:
                coupling_copies[slot].wait()
            both = product(turned[...], wide[:, spot], ((1,), (0,)))
            high, low = two_parts(both[:load_width] + both[load_width:])
            inner[slot, pl.ds(0, load_width)] = high
            inner[slot, pl.ds(load_width, load_width)] = low
        for slot in range(slots):
            spot = pl.ds(trace_width + slot * inner_width, inner_width)
            if first:
                inverse_copies[slot].wait()
            both = product(inv[slot], inner[slot], ((1,), (1,)))
            high, low = two_parts((both[:, :load_width] + both[:, load_width:]) * live[slot])
            factors[spot, pl.ds(0, load_width)] = high
            factors[spot, pl.ds(load_width, load_width)] = low
        if first:
            copies[2].wait()
        both = product(wide[...], factors[...], ((1,), (0,)))
        return both[:, :load_width] + both[:, load_width:]

    def residual_of(step, coupled):
        residual_out[...] = bound[...] - coupled - penalty_weight * held[...]
        wait_arrived(step)
        for face in range(4):
            spot = pl.ds(face * mode_width, mode_width)
            residual_out[spot] = residual_out[spot] + penalty_weight * landed[step, face]

    def advance(step, old_weight, new_weight):
        wait_sent(step)
        change = new_weight * residual_out[...]
        if old_weight is not None:
            change = change + old_weight * direction[...]
        direction[...] = change
        traces = held[...] + change
        held[...] = traces
        for route in routes:
            send(step + 1, route)
        keep_parts(held[...])

    weights = sweep_weights()

    copies[0].wait()
    for route in routes:
        send(0, route)
    keep_parts(held[...])
    coupled = apply(True)
    copies[1].wait()
    residual_of(0, coupled)
    advance(0, None, weights[0][1])

    def sweep(step, carry):
        residual_of(step, apply(False))

        @pl.when(step < SWEEPS)
        def _():
            old_weight, new_weight = weights[-1]
            for index in range(SWEEPS - 1, 0, -1):
                old_weight = jnp.where(step == index, weights[index][0], old_weight)
                new_weight = jnp.where(step == index, weights[index][1], new_weight)
            advance(step, old_weight, new_weight)

        return carry

    lax.fori_loop(1, SWEEPS + 1, sweep, 0)
    wait_sent(SWEEPS)
    traces_out[...] = held[...]


def on_device(
    axis_sizes, coupling, interior_inverse, boundary_stiffness, block_counts, initial_traces, trace_loads
):
    slots, trace_width, inner_width = coupling.shape[2:]
    load_width = initial_traces.shape[-1]
    mode_width = trace_width // FACES
    live = jnp.where(jnp.arange(slots) < block_counts[0, 0], -1.0, 0.0).astype(jnp.float32)
    whole = pl.BlockSpec(memory_space=pl.ANY)
    out = jax.ShapeDtypeStruct((trace_width, load_width), jnp.float32)
    wide_width = trace_width + slots * inner_width
    traces, residual = pl.pallas_call(
        functools.partial(kernel, axis_sizes),
        out_shape=(out, out),
        in_specs=[whole, whole, whole, pl.BlockSpec(memory_space=pltpu.SMEM), whole, whole],
        out_specs=(pl.BlockSpec(memory_space=pltpu.VMEM),) * 2,
        scratch_shapes=[
            pltpu.VMEM((trace_width, wide_width), jnp.bfloat16),
            pltpu.VMEM((slots, inner_width, inner_width), jnp.bfloat16),
            pltpu.VMEM((wide_width, 2 * load_width), jnp.bfloat16),
            pltpu.VMEM((2 * load_width, trace_width), jnp.bfloat16),
            pltpu.VMEM((slots, 2 * load_width, inner_width), jnp.bfloat16),
            pltpu.VMEM((trace_width, load_width), jnp.float32),
            pltpu.VMEM((trace_width, load_width), jnp.float32),
            pltpu.VMEM((trace_width, load_width), jnp.float32),
            pltpu.VMEM((SWEEPS + 1, 4, mode_width, load_width), jnp.float32),
            pltpu.SemaphoreType.DMA((3 + 2 * slots,)),
            pltpu.SemaphoreType.DMA((4,)),
            pltpu.SemaphoreType.DMA((SWEEPS + 1, 4)),
        ],
        compiler_params=pltpu.CompilerParams(
            collective_id=0, has_side_effects=True, vmem_limit_bytes=48 << 20
        ),
        name="condense_and_sweep",
    )(
        coupling[0, 0],
        interior_inverse[0, 0],
        boundary_stiffness[0, 0],
        live,
        initial_traces[0, 0],
        trace_loads[0, 0],
    )
    return (traces[None, None], residual[None, None])


def solution(mesh):
    in_specs = (
        P("gx", ("gy", "ha"), None, None, None),
        P("gx", ("gy", "ha"), None, None, None),
        P("gx", ("gy", "ha"), None, None),
        P("gx", ("gy", "ha")),
        P("gx", ("gy", "ha"), None, None),
        P("gx", ("gy", "ha"), None, None),
    )
    out_specs = (P("gx", ("gy", "ha"), None, None), P("gx", ("gy", "ha"), None, None))
    axis_sizes = (mesh.shape["gx"], mesh.shape["gy"], mesh.shape["ha"])
    return jax.shard_map(
        functools.partial(on_device, axis_sizes),
        mesh=mesh, in_specs=in_specs, out_specs=out_specs, check_vma=False,
    )
```

```python
import functools

import jax
import jax.numpy as jnp
from jax import lax
from jax.experimental import pallas as pl
from jax.experimental.pallas import tpu as pltpu
from jax.sharding import PartitionSpec as P

SWEEPS = 3
FACES = 6

penalty_weight = 2.0
lower_bound = 1.0
upper_bound = 14.0
spectrum_centre = (upper_bound + lower_bound) / 2.0
spectrum_half = (upper_bound - lower_bound) / 2.0
sigma_ratio = spectrum_centre / spectrum_half


def sweep_weights():
    weights = [(0.0, 1.0 / spectrum_centre)]
    weight_old = 1.0 / sigma_ratio
    for _ in range(SWEEPS - 1):
        weight_new = 1.0 / (2.0 * sigma_ratio - weight_old)
        weights.append((weight_new * weight_old, 2.0 * weight_new / spectrum_half))
        weight_old = weight_new
    return weights


def two_parts(value):
    high = value.astype(jnp.bfloat16)
    low = (value - high.astype(jnp.float32)).astype(jnp.bfloat16)
    return high, low


def product(left, right, dims):
    return lax.dot_general(left, right, (dims, ((), ())), preferred_element_type=jnp.float32)


def kernel(
    axis_sizes,
    coupling,
    inverse,
    stiffness,
    counts,
    initial,
    loads,
    traces_out,
    residual_out,
    wide,
    inv,
    factors,
    turned,
    inner,
    held,
    bound,
    direction,
    landed,
    in_sems,
    send_sems,
    recv_sems,
):
    slots, trace_width, inner_width = coupling.shape
    load_width = initial.shape[1]
    mode_width = trace_width // FACES
    rows, groups, halves = axis_sizes
    columns = groups * halves
    row = lax.axis_index("gx")
    column = lax.axis_index("gy") * halves + lax.axis_index("ha")

    def column_id(index):
        return {"gy": lax.div(index, halves), "ha": lax.rem(index, halves)}

    routes = (
        (1, 0, row + 1 < rows, {"gx": row + 1}),
        (0, 1, row > 0, {"gx": row - 1}),
        (3, 2, column + 1 < columns, column_id(column + 1)),
        (2, 3, column > 0, column_id(column - 1)),
    )
    arrivals = ((0, row > 0), (1, row + 1 < rows), (2, column > 0), (3, column + 1 < columns))

    copies = [
        pltpu.make_async_copy(initial, held, in_sems.at[0]),
        pltpu.make_async_copy(loads, bound, in_sems.at[1]),
        pltpu.make_async_copy(stiffness, wide.at[:, pl.ds(0, trace_width)], in_sems.at[2]),
    ]
    coupling_copies, inverse_copies = [], []
    for slot in range(slots):
        spot = pl.ds(trace_width + slot * inner_width, inner_width)
        coupling_copies.append(
            pltpu.make_async_copy(coupling.at[slot], wide.at[:, spot], in_sems.at[3 + slot])
        )
        inverse_copies.append(
            pltpu.make_async_copy(inverse.at[slot], inv.at[slot], in_sems.at[3 + slots + slot])
        )
    copies[0].start()
    for copy in coupling_copies + inverse_copies:
        copy.start()
    copies[2].start()
    copies[1].start()

    barrier = pltpu.get_barrier_semaphore()
    partners = 0
    for _, _, exists, target in routes:
        partners = partners + exists.astype(jnp.int32)

        @pl.when(exists)
        def _():
            pl.semaphore_signal(barrier, inc=1, device_id=target, device_id_type=pl.DeviceIdType.MESH)

    for face, exists in arrivals:

        @pl.when(jnp.logical_not(exists))
        def _():
            landed[:, face] = jnp.zeros((SWEEPS + 1, mode_width, load_width), jnp.float32)

    pl.semaphore_wait(barrier, partners)

    def outgoing(step, route):
        face, spot, _, target = route
        return pltpu.make_async_remote_copy(
            src_ref=held.at[pl.ds(face * mode_width, mode_width)],
            dst_ref=landed.at[step, spot],
            send_sem=send_sems.at[face],
            recv_sem=recv_sems.at[step, spot],
            device_id=target,
            device_id_type=pl.DeviceIdType.MESH,
        )

    def send(step, route):
        @pl.when(route[2])
        def _():
            outgoing(step, route).start()

    def wait_sent(step):
        for route in routes:

            @pl.when(route[2])
            def _():
                outgoing(step, route).wait_send()

    def wait_arrived(step):
        for (face, exists), route in zip(arrivals, routes):

            @pl.when(exists)
            def _():
                outgoing(step, route).wait_recv()

    def keep_parts(traces):
        high, low = two_parts(traces)
        factors[pl.ds(0, trace_width), pl.ds(0, load_width)] = high
        factors[pl.ds(0, trace_width), pl.ds(load_width, load_width)] = low
        high, low = two_parts(traces.T)
        turned[pl.ds(0, load_width)] = high
        turned[pl.ds(load_width, load_width)] = low

    def apply(first):
        @pl.when(first)
        def _():
            for copy in coupling_copies:
                copy.wait()

        for slot in range(slots):
            spot = pl.ds(trace_width + slot * inner_width, inner_width)
            both = product(turned[...], wide[:, spot], ((1,), (0,)))
            high, low = two_parts(both[:load_width] + both[load_width:])
            inner[slot, pl.ds(0, load_width)] = high
            inner[slot, pl.ds(load_width, load_width)] = low

        @pl.when(first)
        def _():
            for copy in inverse_copies + copies[1:]:
                copy.wait()

        for slot in range(slots):
            spot = pl.ds(trace_width + slot * inner_width, inner_width)
            both = product(inv[slot], inner[slot], ((1,), (1,)))
            high, low = two_parts((both[:, :load_width] + both[:, load_width:]) * jnp.where(counts[0, 0] > slot, -1.0, 0.0))
            factors[spot, pl.ds(0, load_width)] = high
            factors[spot, pl.ds(load_width, load_width)] = low
        both = product(wide[...], factors[...], ((1,), (0,)))
        return both[:, :load_width] + both[:, load_width:]

    def residual_of(step, coupled):
        residual_out[...] = bound[...] - coupled - penalty_weight * held[...]
        wait_arrived(step)
        for face in range(4):
            spot = pl.ds(face * mode_width, mode_width)
            residual_out[spot] = residual_out[spot] + penalty_weight * landed[step, face]

    def advance(step, old_weight, new_weight):
        wait_sent(step)
        change = new_weight * residual_out[...] + old_weight * direction[...]
        direction[...] = change
        traces = held[...] + change
        held[...] = traces
        for route in routes:
            send(step + 1, route)
        keep_parts(held[...])

    weights = sweep_weights()

    copies[0].wait()
    for route in routes:
        send(0, route)
    keep_parts(held[...])
    direction[...] = jnp.zeros_like(direction)

    def sweep(step, carry):
        residual_of(step, apply(step == 0))

        @pl.when(step < SWEEPS)
        def _():
            old_weight, new_weight = weights[-1]
            for index in range(SWEEPS - 1):
                old_weight = jnp.where(step == index, weights[index][0], old_weight)
                new_weight = jnp.where(step == index, weights[index][1], new_weight)
            advance(step, old_weight, new_weight)

        return carry

    lax.fori_loop(0, SWEEPS + 1, sweep, 0)
    wait_sent(SWEEPS)
    traces_out[...] = held[...]


def on_device(
    axis_sizes, coupling, interior_inverse, boundary_stiffness, block_counts, initial_traces, trace_loads
):
    slots, trace_width, inner_width = coupling.shape[2:]
    load_width = initial_traces.shape[-1]
    mode_width = trace_width // FACES
    whole = pl.BlockSpec(memory_space=pltpu.HBM)
    out = jax.ShapeDtypeStruct((trace_width, load_width), jnp.float32)
    wide_width = trace_width + slots * inner_width
    traces, residual = pl.pallas_call(
        functools.partial(kernel, axis_sizes),
        out_shape=(out, out),
        in_specs=[whole, whole, whole, pl.BlockSpec(memory_space=pltpu.SMEM), whole, whole],
        out_specs=(pl.BlockSpec(memory_space=pltpu.VMEM),) * 2,
        scratch_shapes=[
            pltpu.VMEM((trace_width, wide_width), jnp.bfloat16),
            pltpu.VMEM((slots, inner_width, inner_width), jnp.bfloat16),
            pltpu.VMEM((wide_width, 2 * load_width), jnp.bfloat16),
            pltpu.VMEM((2 * load_width, trace_width), jnp.bfloat16),
            pltpu.VMEM((slots, 2 * load_width, inner_width), jnp.bfloat16),
            pltpu.VMEM((trace_width, load_width), jnp.float32),
            pltpu.VMEM((trace_width, load_width), jnp.float32),
            pltpu.VMEM((trace_width, load_width), jnp.float32),
            pltpu.VMEM((SWEEPS + 1, 4, mode_width, load_width), jnp.float32),
            pltpu.SemaphoreType.DMA((3 + 2 * slots,)),
            pltpu.SemaphoreType.DMA((4,)),
            pltpu.SemaphoreType.DMA((SWEEPS + 1, 4)),
        ],
        compiler_params=pltpu.CompilerParams(
            collective_id=0, has_side_effects=True, vmem_limit_bytes=67043328
        ),
        name="condense_and_sweep",
    )(
        coupling[0, 0],
        interior_inverse[0, 0],
        boundary_stiffness[0, 0],
        block_counts,
        initial_traces[0, 0],
        trace_loads[0, 0],
    )
    return (traces[None, None], residual[None, None])


def solution(mesh):
    in_specs = (
        P("gx", ("gy", "ha"), None, None, None),
        P("gx", ("gy", "ha"), None, None, None),
        P("gx", ("gy", "ha"), None, None),
        P("gx", ("gy", "ha")),
        P("gx", ("gy", "ha"), None, None),
        P("gx", ("gy", "ha"), None, None),
    )
    out_specs = (P("gx", ("gy", "ha"), None, None), P("gx", ("gy", "ha"), None, None))
    axis_sizes = (mesh.shape["gx"], mesh.shape["gy"], mesh.shape["ha"])
    return jax.shard_map(
        functools.partial(on_device, axis_sizes),
        mesh=mesh, in_specs=in_specs, out_specs=out_specs, check_vma=False,
    )
```
